256 devices in a mesh: facet: 64 (over z, y, core), col: 4 (over x).
Axes of the slice: x: 4, y: 4, z: 8, core: 2. Of those that a mesh axis runs over, the one named last changes fastest.
Arguments:
- strip: bfloat16 [2, 64, 262144], P(None, None, 'facet'), may hold values from -6 to 6
- screen_first: bfloat16 [2, 512, 512], replicated, may hold values from -1 to 1
- screen_second: bfloat16 [2, 512, 512], replicated, may hold values from -1 to 1
- owners: int32 [4, 4096, 3], P('col', 'facet'), may hold values from 0 to 127, all different within a row; in each aligned block of 64 rows (0 to 63, 64 to 127, ..., all dimensions but the last counted through in order) at most 2 rows name the same one
- live: int32 [4, 4096, 3], P('col', 'facet'), may hold values 0 or 1
- place: int32 [4, 4096, 3], P('col', 'facet'), may hold values from 0 to 63
Outputs:
- facet_image: float32 [2, 64, 262144], P(None, None, ('facet', 'col'))
The draws below stay inside these ranges and needn't reach their ends.
Inputs may be any that keep to these rules, and one draw needn't show every extreme that they name: `owners`: each row names three different subgrids; among the rows of one device no subgrid is named more than 2 times, a bound that some block reaches. `place`: tile p lies at tile row p // 8 and tile column p % 8.
All inputs are finite; a program needn't handle non-finite values. No bound on the sum of `live` on one device may be relied on, other than what follows from the above.
Results may differ from the reference program's by a relative error of at most 0.013.
Values may be sent and summed in bfloat16 or wider, within the bound.
No kernel may reach another device: no remote copies, remote signals or barrier semaphores. Data moves between devices by JAX's collectives and lax.ppermute only.
A program may use at most 64 MiB of HBM per device.

```python
import math
import jax
import jax.numpy as jnp
import numpy as np
from jax import lax

WIN = 64
SUB = 512
WIN_DEV = 64
POS = 64
WINDOWS = 4096
SUBGRIDS = 128
COLS = 4
CAP = 2
N_COL = 4


def place_ends(drawn, stream_key, least, high):
    extent = drawn.shape
    index_at = [jax.random.randint(jax.random.fold_in(stream_key, axis), (), 0, extent[axis]) for axis in range(len(extent))]
    drawn = drawn.at[tuple(index_at)].set(least)
    longest = extent.index(max(extent))
    index_at[longest] = (index_at[longest] + 1) % extent[longest]
    return drawn.at[tuple(index_at)].set(high)


def shard_levels(own_key, shape, shards, low, top_value):
    gain = 1.0
    for position, shards_of in shards:
        steps = jax.random.uniform(jax.random.fold_in(jax.random.fold_in(own_key, 6), position), (shards_of,), jnp.float32, low / len(shards), top_value / len(shards))
        gain = gain * jnp.repeat(jnp.exp(steps), shape[position] // shards_of).reshape((-1,) + (1,) * (len(shape) - 1 - position))
    return gain


def deal_out(key, own, number, rows, count, top, limit, slope):
    ranking = jax.random.permutation(key, count)
    crowded, usual = load_shares(count, rows * top, limit, slope, True), load_shares(count, rows * top, limit, slope, False)
    places = jnp.arange(count)

    def named(lengths, offset_by):
        used = int((lengths > 0).sum())
        fixed = max(1, used // 4)
        moved = fixed + (places - fixed + offset_by * (used - fixed)) % max(1, count - fixed)
        return jnp.zeros((count,), jnp.int32).at[ranking[jnp.where(places < fixed, places, moved)]].set(jnp.asarray(lengths, jnp.int32))

    lengths = jnp.where(number % 4 == 0, named(crowded, number // 4), named(usual, number - number // 4 - 1))
    mixed = jax.random.permutation(jax.random.fold_in(own, 3), count)
    source_of, receiver = mixed[0:count // 2 * 2:2], mixed[1:count // 2 * 2:2]
    slack = jnp.minimum(lengths[source_of] - 1, limit - lengths[receiver]) // 2
    slack = jnp.where((source_of == ranking[0]) | (receiver == ranking[0]) | (lengths[receiver] == 0), 0, jnp.maximum(slack, 0))
    moved = jax.random.randint(jax.random.fold_in(own, 4), (count // 2,), 0, 1 << 20) % (slack + 1)
    lengths = lengths.at[source_of].add(-moved).at[receiver].add(moved)
    members = jnp.searchsorted(jnp.cumsum(lengths), jnp.arange(rows * top), side="right").astype(jnp.int32)
    table = members.reshape(top, rows).T
    table = table[jax.random.permutation(jax.random.fold_in(own, 1), rows)]
    offset_by = jax.random.randint(jax.random.fold_in(own, 2), (rows, 1), 0, top)
    return jnp.take_along_axis(table, (jnp.arange(top)[None, :] + offset_by) % top, axis=1)


def load_shares(amount, total, most, skew, full):
    portions = [(1 << 20) // math.isqrt(standing ** skew) + 1 for standing in range(1, amount + 1)]
    largest = most if full else min(most, max(-(-total // amount), total * portions[0] // sum(portions)))
    least = 1 if total - largest >= amount - 1 else 0
    counts, rest = [largest] + [least] * (amount - 1), total - largest - least * (amount - 1)
    while rest > 0:
        candidates = [i for i in range(1, amount) if counts[i] < largest] or [i for i in range(1, amount) if counts[i] < most]
        mass, remaining = sum([portions[i] for i in candidates]), rest
        for i in candidates:
            extra = min(most - counts[i], max(1, remaining * portions[i] // mass), rest)
            counts[i] = counts[i] + extra
            rest = rest - extra
    return np.array(counts)


def scatter_about(own_key, dims, deviation, limit, split=(), kind=jnp.bfloat16):
    entries = jax.random.normal(own_key, dims, jnp.float32) * deviation
    if len(split) > 0:
        entries = shard_levels(own_key, dims, split, -0.22, 0.18) * entries
    return jnp.clip(entries, min=-limit, max=limit).astype(kind)


def setup_inputs(seed: int = 0) -> dict:
    splits = jax.random.split(jax.random.key(seed), 7)
    strip = scatter_about(splits[0], (2, WIN, WINDOWS * WIN), 1.0, 6.0, ((2, 64),))
    screen_first = jnp.clip(jax.random.uniform(splits[1], (2, SUB, SUB), jnp.float32, -1.0, 1.0), -1.0, 1.0).astype(jnp.bfloat16)
    screen_second = jnp.clip(jax.random.uniform(splits[2], (2, SUB, SUB), jnp.float32, -1.0, 1.0), -1.0, 1.0).astype(jnp.bfloat16)
    owners_keys = jax.random.split(jax.random.fold_in(splits[3], 1), COLS * WINDOWS // WIN_DEV)
    owners_turns = jax.random.permutation(jax.random.fold_in(splits[3], 3), COLS * WINDOWS // WIN_DEV)
    owners = jax.vmap(lambda own, number: deal_out(jax.random.fold_in(splits[3], 2), own, number, WIN_DEV, SUBGRIDS, 3, CAP, 1))(owners_keys, owners_turns).reshape((COLS, WINDOWS, 3))
    live = place_ends((jax.random.randint(splits[4], (COLS, WINDOWS, 3), 0, 3) < 2).astype(jnp.int32), jax.random.fold_in(splits[4], 1), 0, 1)
    place = place_ends(jax.random.randint(splits[5], (COLS, WINDOWS, 3), 0, POS), jax.random.fold_in(splits[5], 1), 0, POS - 1).astype(jnp.int32)
    return dict(strip=strip, screen_first=screen_first, screen_second=screen_second, owners=owners, live=live, place=place)


def dft_table(length, direction):
    index = jnp.arange(length, dtype=jnp.int32)
    phase = index[:, None] * index[None, :] % length
    angle = phase.astype(jnp.float32) * (2.0 * math.pi / length)
    scale = 1.0 / math.sqrt(length)
    return (jnp.cos(angle) * scale, direction * jnp.sin(angle) * scale)

def left_apply(table, field):
    real_table, imag_table = table
    real_part, imag_part = field
    real = jnp.dot(real_table, real_part, preferred_element_type=jnp.float32) - jnp.dot(imag_table, imag_part, preferred_element_type=jnp.float32)
    imag = jnp.dot(real_table, imag_part, preferred_element_type=jnp.float32) + jnp.dot(imag_table, real_part, preferred_element_type=jnp.float32)
    return (real, imag)

def right_apply(field, table):
    real_table, imag_table = table
    real_part, imag_part = field
    real = jnp.dot(real_part, real_table, preferred_element_type=jnp.float32) - jnp.dot(imag_part, imag_table, preferred_element_type=jnp.float32)
    imag = jnp.dot(real_part, imag_table, preferred_element_type=jnp.float32) + jnp.dot(imag_part, real_table, preferred_element_type=jnp.float32)
    return (real, imag)

def screen_apply(field, screen):
    real_part, imag_part = field
    screen_real = screen[0].astype(jnp.float32)
    screen_imag = screen[1].astype(jnp.float32)
    real = real_part * screen_real - imag_part * screen_imag
    imag = real_part * screen_imag + imag_part * screen_real
    return (real.astype(jnp.bfloat16), imag.astype(jnp.bfloat16))

def process_tiles(tiles, screen_first, screen_second, forward, inverse):
    tile_count, width = tiles.shape
    side_tiles = math.isqrt(tile_count)
    win_size = math.isqrt(width // 2)
    sub_size = side_tiles * win_size
    field = tiles.reshape(side_tiles, side_tiles, 2, win_size, win_size).transpose(2, 0, 3, 1, 4).reshape(2, sub_size, sub_size)
    rows = left_apply(forward, (field[0], field[1]))
    rows = (rows[0].astype(jnp.bfloat16), rows[1].astype(jnp.bfloat16))
    spectrum = screen_apply(right_apply(rows, forward), screen_first)
    back = left_apply(inverse, spectrum)
    back = (back[0].astype(jnp.bfloat16), back[1].astype(jnp.bfloat16))
    image = screen_apply(right_apply(back, inverse), screen_second)
    stacked = jnp.stack([image[0], image[1]])
    return stacked.reshape(2, side_tiles, win_size, side_tiles, win_size).transpose(1, 3, 0, 2, 4).reshape(tile_count, width)

def reference(strip, screen_first, screen_second, owners, live, place):
    width = 2 * WIN * WIN
    small_real, small_imag = dft_table(WIN, -1.0)
    small = (small_real.astype(jnp.bfloat16), small_imag.astype(jnp.bfloat16))
    front = left_apply(small, (strip[0], strip[1]))
    contrib = jnp.stack([front[0], front[1]]).astype(jnp.bfloat16)
    windows = contrib.reshape(2, WIN, WINDOWS, WIN).transpose(2, 0, 1, 3).reshape(WINDOWS, width)
    big_real, big_imag = dft_table(SUB, -1.0)
    forward = (big_real.astype(jnp.bfloat16), big_imag.astype(jnp.bfloat16))
    inverse = (big_real.astype(jnp.bfloat16), (-big_imag).astype(jnp.bfloat16))
    widened = windows.astype(jnp.float32)
    summed = jnp.zeros((WINDOWS, width), jnp.float32)
    for column in range(N_COL):
        target = (owners[column] * POS + place[column]).astype(jnp.int32)
        weight = live[column].astype(jnp.float32)
        embedded = jnp.zeros((SUBGRIDS * POS, width), jnp.float32)
        for member in range(3):
            embedded = embedded + jax.ops.segment_sum(widened * weight[:, member, None], target[:, member], num_segments=SUBGRIDS * POS)
        tiles = embedded.astype(jnp.bfloat16).reshape(SUBGRIDS, POS, width)
        processed = lax.map(lambda block: process_tiles(block, screen_first, screen_second, forward, inverse), tiles)
        flat = processed.reshape(SUBGRIDS * POS, width)
        for member in range(3):
            summed = summed + flat[target[:, member]].astype(jnp.float32) * weight[:, member, None]
    field = summed.reshape(WINDOWS, 2, WIN, WIN).transpose(1, 2, 0, 3).reshape(2, WIN, WINDOWS * WIN)
    back_real, back_imag = dft_table(WIN, 1.0)
    highest = lax.Precision.HIGHEST
    real = jnp.dot(back_real, field[0], precision=highest) - jnp.dot(back_imag, field[1], precision=highest)
    imag = jnp.dot(back_real, field[1], precision=highest) + jnp.dot(back_imag, field[0], precision=highest)
    return jnp.stack([real, imag])
```

```python
import functools
import math

import jax
import jax.numpy as jnp
import numpy as np
from jax import lax
from jax.experimental import pallas as pl
from jax.experimental.pallas import tpu as pltpu
from jax.sharding import Mesh, PartitionSpec as P

NZ, NY, NK, NX = 8, 4, 2, 4
WIN = 64
QUARTER = WIN // NX
SUB = 512
SIDE = SUB // WIN
TILES = SIDE * SIDE
CAP = 2
LOCAL = 2
SOURCES = NY * NK
PEERS = SOURCES * NX
SLOTS = NZ * CAP
LANES = 128
BF, F32 = jnp.bfloat16, jnp.float32


def dft(length):
    index = np.arange(length)
    angle = ((index[:, None] * index[None, :]) % length).astype(np.float32) * np.float32(
        2.0 * math.pi / length
    )
    scale = np.float32(1.0 / math.sqrt(length))
    return (
        (np.cos(angle) * scale).astype(np.float32),
        (-np.sin(angle) * scale).astype(np.float32),
    )


def front_table():
    real, imag = dft(WIN)
    both = np.stack(
        [np.concatenate([real, -imag], 1), np.concatenate([imag, real], 1)]
    )
    cut = both.reshape(2, NX, QUARTER, 2 * WIN).transpose(1, 0, 2, 3)
    return cut.reshape(NX, 2 * QUARTER, 2 * WIN).astype(BF)


def left_table():
    real, imag = dft(SUB)
    return np.concatenate([real, imag], 1).astype(BF)


def right_table():
    real, imag = dft(SUB)
    full = np.stack([np.stack([real, imag]), np.stack([-imag, real])])
    full = full.reshape(2, 2, SIDE, WIN, SUB // LANES, LANES)
    return full.transpose(2, 0, 3, 4, 1, 5).reshape(2 * SUB, 2 * SUB).astype(BF)


def last_table():
    real, imag = dft(WIN)
    return np.concatenate([real, -imag], 0).astype(np.float32)


def swap_halves(x):
    return pltpu.roll(x, WIN, x.ndim - 1)


def low_half(shape):
    return lax.broadcasted_iota(jnp.int32, shape, len(shape) - 1) < WIN


def front_kernel(where_ref, table_ref, strip_ref, out_ref):
    table = table_ref[where_ref[0]]
    for j in range(WIN // 2):
        cols = pl.ds(j * LANES, LANES)
        block = jnp.concatenate([strip_ref[0, :, cols], strip_ref[1, :, cols]], 0)
        both = jnp.dot(table, block, preferred_element_type=F32)
        real, imag = both[:QUARTER], both[QUARTER:]
        low = low_half(real.shape)
        out_ref[2 * j] = jnp.where(low, real, swap_halves(imag)).astype(BF)
        out_ref[2 * j + 1] = jnp.where(low, swap_halves(real), imag).astype(BF)


def pack_kernel(extra, rows_ref, *refs):
    blocks, out_ref = list(refs[:9]), refs[-2]
    middle_ref = refs[-1]
    middle_ref[: WIN // 2] = blocks[7][...]
    middle_ref[WIN // 2 :] = blocks[8][...]
    blocks = blocks[:4] + [middle_ref] + blocks[4:7]

    def step(d, carry):
        for j in range(NZ):
            for cap in range(CAP):
                slot = j * CAP + cap
                out_ref[d, slot] = blocks[j][rows_ref[d * SLOTS + slot]]
        if extra:
            out_ref[d, SLOTS] = refs[9][d]
        return carry

    lax.fori_loop(0, PEERS, step, 0, unroll=2)


def subgrid_kernel(
    tags_ref, left_ref, right_ref, first_ref, second_ref, slabs_ref, out_ref,
    acc_ref, twin_ref, row_ref, tile_ref,
):
    acc_ref[...] = jnp.zeros(acc_ref.shape, F32)

    def embed(i, carry):
        tag = tags_ref[i]
        source = i // SLOTS
        slot = i % SLOTS
        for q in range(NX):
            rows = pl.ds(q * QUARTER, QUARTER)
            acc_ref[tag, rows, :] += slabs_ref[source * NX + q, slot].astype(F32)
        return carry

    lax.fori_loop(0, SOURCES * SLOTS, embed, 0, unroll=4)

    for t in range(SIDE):
        cols = pl.ds(t * LANES, LANES)
        panel = acc_ref[t * SIDE : (t + 1) * SIDE].reshape(SUB, LANES)
        turned = swap_halves(panel)
        twin_ref[:SUB, cols] = panel.astype(BF)
        twin_ref[SUB:, cols] = jnp.where(low_half(panel.shape), -turned, turned).astype(BF)

    step = 2 * LANES
    count = 2 * SUB // step
    for n in range(count):
        cols = pl.ds(n * step, step)
        row_ref[:, cols] = jnp.dot(
            left_ref[...], twin_ref[:, cols], preferred_element_type=F32
        ).astype(BF)
    for n in range(count):
        cols = pl.ds(n * step, step)
        half = pl.ds(n * LANES, LANES)
        got = jnp.dot(row_ref[...], right_ref[:, cols], preferred_element_type=F32)
        real, imag = got[:, :LANES], got[:, LANES:]
        screen_real = first_ref[0, :, half].astype(F32)
        screen_imag = first_ref[1, :, half].astype(F32)
        new_real = (real * screen_real - imag * screen_imag).astype(BF)
        new_imag = (real * screen_imag + imag * screen_real).astype(BF)
        lower = pl.ds(n * step, LANES)
        upper = pl.ds(n * step + LANES, LANES)
        twin_ref[:SUB, lower] = new_real
        twin_ref[:SUB, upper] = new_imag
        twin_ref[SUB:, lower] = new_imag
        twin_ref[SUB:, upper] = -new_real
    for n in range(count):
        cols = pl.ds(n * step, step)
        row_ref[:, cols] = jnp.dot(
            left_ref[...], twin_ref[:, cols], preferred_element_type=F32
        ).astype(BF)
    tile_ref[TILES] = jnp.zeros((WIN, LANES), BF)
    for n in range(count):
        got = lax.dot_general(
            row_ref[...],
            right_ref[pl.ds(n * step, step), :],
            (((1,), (1,)), ((), ())),
            preferred_element_type=F32,
        )
        cols = pl.ds(n * LANES, LANES)
        screen_real = second_ref[0, :, cols].astype(F32)
        screen_imag = second_ref[1, :, cols].astype(F32)
        real_turned, imag_turned = swap_halves(screen_real), swap_halves(screen_imag)
        low = low_half(screen_real.shape)
        for h in range(2):
            part = got[:, h * LANES : (h + 1) * LANES]
            if h == 0:
                keep = jnp.where(low, screen_real, real_turned)
                cross = jnp.where(low, -screen_imag, imag_turned)
            else:
                keep = jnp.where(low, real_turned, screen_real)
                cross = jnp.where(low, -imag_turned, screen_imag)
            done = (part * keep + swap_halves(part) * cross).astype(BF)
            t = 2 * n + h
            tile_ref[t * SIDE : (t + 1) * SIDE] = done.reshape(SIDE, WIN, LANES)

    def cut(i, carry):
        tag = tags_ref[i]
        source = i // SLOTS
        slot = i % SLOTS
        for q in range(NX):
            out_ref[source * NX + q, slot] = tile_ref[tag, pl.ds(q * QUARTER, QUARTER), :]
        return carry

    lax.fori_loop(0, SOURCES * SLOTS, cut, 0, unroll=4)


def add_slots(rows_ref, slots_ref, accs):
    def step(d, carry):
        for cap in range(CAP):
            for j in range(NZ):
                slot = j * CAP + cap
                row = rows_ref[d * SLOTS + slot]
                accs[j][row] += slots_ref[d, slot].astype(F32)
        return carry

    lax.fori_loop(0, PEERS, step, 0)


def sum_first_kernel(rows_ref, slots_ref, *accs):
    for acc in accs:
        acc[...] = jnp.zeros(acc.shape, F32)
    add_slots(rows_ref, slots_ref, accs)


def sum_second_kernel(rows_ref, slots_ref, *refs):
    before, outs, accs = refs[:NZ], refs[NZ : 2 * NZ], refs[2 * NZ :]
    for acc, start in zip(accs, before):
        acc[...] = start[...]
    add_slots(rows_ref, slots_ref, accs)
    for acc, out in zip(accs, outs):
        out[...] = acc[:WIN].astype(BF)


def last_kernel(where_ref, table_ref, *refs):
    blocks, out_ref, tile_ref = refs[:NX], refs[NX], refs[NX + 1]
    count = WIN // NX
    for s in range(NX):
        q = (where_ref[0] + NX - s) % NX
        rows = pl.ds(pl.multiple_of(q * QUARTER, QUARTER), QUARTER)
        for w in range(count):
            tile_ref[w, rows, :] = blocks[s][w].astype(F32)
    for j in range(count // 2):
        ends = []
        for h in range(2):
            both = jnp.dot(
                table_ref[...],
                tile_ref[2 * j + h],
                precision=lax.Precision.HIGHEST,
                preferred_element_type=F32,
            )
            turned = swap_halves(both[WIN:])
            ends.append(both[:WIN] + jnp.where(low_half(turned.shape), -turned, turned))
        even, odd = ends
        low = low_half(even.shape)
        cols = pl.ds(j * LANES, LANES)
        out_ref[0, :, cols] = jnp.where(low, even, swap_halves(odd))
        out_ref[1, :, cols] = jnp.where(low, swap_halves(even), odd)


VMEM = pl.BlockSpec(memory_space=pltpu.VMEM)
SMEM = pl.BlockSpec(memory_space=pltpu.SMEM)


def call(kernel, specs, out, scratch=(), flops=0, moved=0):
    outs = jax.tree.map(lambda _: VMEM, out)
    return pl.pallas_call(
        kernel,
        in_specs=list(specs),
        out_specs=outs,
        out_shape=out,
        scratch_shapes=list(scratch),
        cost_estimate=pl.CostEstimate(flops=flops, bytes_accessed=moved, transcendentals=0),
        compiler_params=pltpu.CompilerParams(vmem_limit_bytes=48 << 20),
    )


def slot_codes(owners, live, place):
    owner, used, tile = owners.reshape(-1), live.reshape(-1), place.reshape(-1)
    entries = owner.shape[0]
    order = jnp.arange(entries, dtype=jnp.int32)
    earlier = (owner[:, None] == owner[None, :]) & (order[:, None] < order[None, :])
    rank = jnp.sum(earlier.astype(jnp.int32), axis=0)
    slot_of = owner * CAP + rank
    code = (order // 3) * TILES + tile + 1
    slots = jnp.arange(NZ * SOURCES * LOCAL * CAP, dtype=jnp.int32)
    hit = (slot_of[None, :] == slots[:, None]) & (used[None, :] == 1)
    return jnp.sum(jnp.where(hit, code[None, :], 0), axis=1) - 1


def shift(value, axis, by):
    size = lax.axis_size(axis)
    return lax.ppermute(value, axis, [(i, (i + by) % size) for i in range(size)])


def pick(rows, index):
    hit = index[:, None] == jnp.arange(rows.shape[0], dtype=jnp.int32)[None, :]
    return jnp.sum(jnp.where(hit[:, :, None], rows[None], 0), axis=1)


def flip(value, axis, bit):
    size = lax.axis_size(axis)
    return lax.ppermute(value, axis, [(i, i ^ bit) for i in range(size)])


def exchange_codes(codes, z, x):
    table = codes.reshape(1, -1)
    for bit in (1, 2, 4):
        other = flip(table, "z", bit)
        table = jnp.concatenate([table, other], 0)
    table = lax.dynamic_index_in_dim(table.reshape(NZ, NZ, -1), z, 1, keepdims=False)
    table = pick(table, (z + jnp.arange(NZ, dtype=jnp.int32)) % NZ ^ z).reshape(1, -1)
    for bit in (1, 2):
        other = flip(table, "x", bit)
        table = jnp.concatenate([table, other], 0)
    table = pick(table, jnp.arange(NX, dtype=jnp.int32) ^ x)
    return table.reshape(NX, NZ, SOURCES, LOCAL, CAP)


def gather_up(own):
    half = WIN // 2
    down, up = [own], [own]
    for _ in range(3):
        up.append(shift(up[-1], "z", 1))
        down.append(shift(down[-1], "z", -1))
    low = shift(up[3][:half], "z", 1)
    high = shift(down[3][half:], "z", -1)
    return down + up[:0:-1] + [low, high]


def add(*terms):
    return sum(t.astype(F32) for t in terms).astype(BF)


def sum_up(parts):
    half = WIN // 2
    low = shift(parts[4][:half], "z", 1)
    high = shift(parts[4][half:], "z", -1)
    up = jnp.concatenate([add(parts[3][:half], low), parts[3][half:]], 0)
    down = jnp.concatenate([parts[5][:half], add(parts[5][half:], high)], 0)
    up, down = shift(up, "z", 1), shift(down, "z", -1)
    up, down = shift(add(parts[2], up), "z", 1), shift(add(parts[6], down), "z", -1)
    up, down = shift(add(parts[1], up), "z", 1), shift(add(parts[7], down), "z", -1)
    return add(parts[0], up, down)


def work(strip, screen_first, screen_second, owners, live, place):
    z, x = lax.axis_index("z"), lax.axis_index("x")
    plane = ("y", "k", "x")
    block = jax.ShapeDtypeStruct((WIN, QUARTER, LANES), BF)
    own = call(
        front_kernel, [SMEM, VMEM, VMEM], block, flops=2 * 32 * 128 * 4096, moved=2 << 20
    )(x.reshape(1), jnp.asarray(front_table()), strip)
    blocks = gather_up(own)

    codes = exchange_codes(slot_codes(owners[0], live[0], place[0]), z, x)
    codes = codes.transpose(3, 2, 0, 1, 4)
    dead = codes < 0
    rows = jnp.where(dead, WIN, codes // TILES).reshape(LOCAL, PEERS * SLOTS)
    taken = jnp.minimum(rows, WIN - 1)
    tags = codes % TILES
    tags = jnp.where(dead, TILES, tags % SIDE * SIDE + tags // SIDE)
    tags = tags.reshape(LOCAL, PEERS, SLOTS).transpose(1, 0, 2).reshape(PEERS, 1, LOCAL * SLOTS)
    extra = jnp.pad(tags.astype(BF), ((0, 0), (0, QUARTER - 1), (0, LANES - LOCAL * SLOTS)))

    left, right = jnp.asarray(left_table()), jnp.asarray(right_table())
    returned = []
    for part in range(LOCAL):
        first = part == 0
        sent = call(
            functools.partial(pack_kernel, first),
            [SMEM] + [VMEM] * (10 if first else 9),
            jax.ShapeDtypeStruct((PEERS, SLOTS + first, QUARTER, LANES), BF),
            scratch=[pltpu.VMEM((WIN, QUARTER, LANES), BF)],
            flops=1 << 28,
            moved=4 << 20,
        )(taken[part], *blocks, *([extra] if first else []))
        got = lax.all_to_all(sent, plane, split_axis=0, concat_axis=0, tiled=True)
        if first:
            spots = got.reshape(SOURCES, NX, SLOTS + 1, QUARTER, LANES)
            spots = spots[:, 0, SLOTS, 0, : LOCAL * SLOTS].astype(jnp.int32)
            spots = spots.reshape(SOURCES, LOCAL, SLOTS).transpose(1, 0, 2)
            spots = spots.reshape(LOCAL, SOURCES * SLOTS)
        done = call(
            subgrid_kernel,
            [SMEM] + [VMEM] * 5,
            jax.ShapeDtypeStruct((PEERS, SLOTS, QUARTER, LANES), BF),
            scratch=[
                pltpu.VMEM((TILES + 1, WIN, LANES), F32),
                pltpu.VMEM((2 * SUB, 2 * SUB), BF),
                pltpu.VMEM((SUB, 2 * SUB), BF),
                pltpu.VMEM((TILES + 1, WIN, LANES), BF),
            ],
            flops=8 * 2 * SUB * SUB * SUB * 2,
            moved=10 << 20,
        )(spots[part], left, right, screen_first, screen_second, got)
        returned.append(lax.all_to_all(done, plane, split_axis=0, concat_axis=0, tiled=True))
    acc = [jax.ShapeDtypeStruct((WIN + 1, QUARTER, LANES), F32)] * NZ
    partial = call(
        sum_first_kernel, [SMEM, VMEM], acc, flops=1 << 28, moved=6 << 20
    )(rows[0], returned[0])
    parts = call(
        sum_second_kernel,
        [SMEM, VMEM] + [VMEM] * NZ,
        [block] * NZ,
        scratch=[pltpu.VMEM((WIN + 1, QUARTER, LANES), F32)] * NZ,
        flops=1 << 28,
        moved=8 << 20,
    )(rows[1], returned[1], *partial)
    mine = sum_up(parts)
    count = WIN // NX
    pieces = []
    for s in range(NX):
        piece = lax.dynamic_slice_in_dim(mine, (x + s) % NX * count, count, 0)
        pieces.append(shift(piece, "x", s) if s else piece)
    return call(
        last_kernel,
        [SMEM] + [VMEM] * (1 + NX),
        jax.ShapeDtypeStruct((2, WIN, count * WIN), F32),
        scratch=[pltpu.VMEM((count, WIN, LANES), F32)],
        flops=1 << 28,
        moved=1 << 20,
    )(x.reshape(1), jnp.asarray(last_table()), *pieces)


def solution(mesh):
    fine = Mesh(mesh.devices.reshape(NZ, NY, NK, NX), ("z", "y", "k", "x"))
    facet = ("z", "y", "k")
    entry = P("x", facet, None)
    return jax.shard_map(
        work,
        mesh=fine,
        in_specs=(P(None, None, facet), P(), P(), entry, entry, entry),
        out_specs=P(None, None, facet + ("x",)),
        check_vma=False,
    )
```

```python
import functools
import math

import jax
import jax.numpy as jnp
import numpy as np
from jax import lax
from jax.experimental import pallas as pl
from jax.experimental.pallas import tpu as pltpu
from jax.sharding import Mesh, PartitionSpec as P

NZ, NY, NK, NX = 8, 4, 2, 4
WIN = 64
QUARTER = WIN // NX
SUB = 512
SIDE = SUB // WIN
TILES = SIDE * SIDE
CAP = 2
LOCAL = 2
SOURCES = NY * NK
PEERS = SOURCES * NX
SLOTS = NZ * CAP
LANES = 128
BF, F32 = jnp.bfloat16, jnp.float32


def dft(length):
    index = np.arange(length)
    angle = ((index[:, None] * index[None, :]) % length).astype(np.float32) * np.float32(
        2.0 * math.pi / length
    )
    scale = np.float32(1.0 / math.sqrt(length))
    return (
        (np.cos(angle) * scale).astype(np.float32),
        (-np.sin(angle) * scale).astype(np.float32),
    )


def front_table():
    real, imag = dft(WIN)
    both = np.stack(
        [np.concatenate([real, -imag], 1), np.concatenate([imag, real], 1)]
    )
    cut = both.reshape(2, NX, QUARTER, 2 * WIN).transpose(1, 0, 2, 3)
    return cut.reshape(NX, 2 * QUARTER, 2 * WIN).astype(BF)


def left_table():
    real, imag = dft(SUB)
    return np.concatenate([real, imag], 1).astype(BF)


def right_table():
    real, imag = dft(SUB)
    full = np.stack([np.stack([real, imag]), np.stack([-imag, real])])
    full = full.reshape(2, 2, SIDE, WIN, SUB // LANES, LANES)
    return full.transpose(2, 0, 3, 4, 1, 5).reshape(2 * SUB, 2 * SUB).astype(BF)


def last_table():
    real, imag = dft(WIN)
    return np.concatenate([real, -imag], 0).astype(np.float32)


def swap_halves(x):
    return pltpu.roll(x, WIN, x.ndim - 1)


def low_half(shape):
    return lax.broadcasted_iota(jnp.int32, shape, len(shape) - 1) < WIN


def front_kernel(where_ref, table_ref, strip_ref, out_ref):
    table = table_ref[where_ref[0]]
    for j in range(WIN // 2):
        cols = pl.ds(j * LANES, LANES)
        block = jnp.concatenate([strip_ref[0, :, cols], strip_ref[1, :, cols]], 0)
        both = jnp.dot(table, block, preferred_element_type=F32)
        real, imag = both[:QUARTER], both[QUARTER:]
        low = low_half(real.shape)
        out_ref[2 * j] = jnp.where(low, real, swap_halves(imag)).astype(BF)
        out_ref[2 * j + 1] = jnp.where(low, swap_halves(real), imag).astype(BF)


def codes_kernel(owner_ref, live_ref, place_ref, out_ref):
    shape = (WIN, NZ * SOURCES * LOCAL)
    window = lax.broadcasted_iota(jnp.int32, shape, 0)
    subgrid = lax.broadcasted_iota(jnp.int32, shape, 1)
    count = jnp.zeros(shape, F32)
    value = jnp.zeros(shape, F32)
    for k in range(3):
        entry = (0, slice(None), slice(k, k + 1))
        hit = owner_ref[entry] == subgrid
        code = (window * TILES + place_ref[entry] + 1).astype(F32)
        count += jnp.where(hit, 1.0, 0.0)
        value += jnp.where(hit & (live_ref[entry] == 1), code, 0.0)
    square = (WIN, WIN)
    earlier = lax.broadcasted_iota(jnp.int32, square, 1) < lax.broadcasted_iota(
        jnp.int32, square, 0
    )
    rank = jnp.dot(
        jnp.where(earlier, 1.0, 0.0).astype(BF), count.astype(BF), preferred_element_type=F32
    )
    for cap in range(CAP):
        mine = jnp.sum(jnp.where(rank == float(cap), value, 0.0), axis=0, keepdims=True)
        out_ref[:, cap * shape[1] : (cap + 1) * shape[1]] = mine.astype(jnp.int32) - 1


def pack_kernel(extra, rows_ref, *refs):
    blocks, out_ref = list(refs[:9]), refs[-2]
    middle_ref = refs[-1]
    middle_ref[: WIN // 2] = blocks[7][...]
    middle_ref[WIN // 2 :] = blocks[8][...]
    blocks = blocks[:4] + [middle_ref] + blocks[4:7]

    def step(d, carry):
        for j in range(NZ):
            for cap in range(CAP):
                slot = j * CAP + cap
                out_ref[d, slot] = blocks[j][rows_ref[d * SLOTS + slot]]
        if extra:
            out_ref[d, SLOTS] = refs[9][d]
        return carry

    lax.fori_loop(0, PEERS, step, 0, unroll=2)


def subgrid_kernel(
    tags_ref, left_ref, right_ref, first_ref, second_ref, slabs_ref, out_ref,
    acc_ref, twin_ref, row_ref, tile_ref,
):
    acc_ref[...] = jnp.zeros(acc_ref.shape, F32)

    def embed(i, carry):
        tag = tags_ref[i]
        source = i // SLOTS
        slot = i % SLOTS
        for q in range(NX):
            rows = pl.ds(q * QUARTER, QUARTER)
            acc_ref[tag, rows, :] += slabs_ref[source * NX + q, slot].astype(F32)
        return carry

    lax.fori_loop(0, SOURCES * SLOTS, embed, 0, unroll=4)

    for t in range(SIDE):
        cols = pl.ds(t * LANES, LANES)
        panel = acc_ref[t * SIDE : (t + 1) * SIDE].reshape(SUB, LANES)
        turned = swap_halves(panel)
        twin_ref[:SUB, cols] = panel.astype(BF)
        twin_ref[SUB:, cols] = jnp.where(low_half(panel.shape), -turned, turned).astype(BF)

    step = 2 * LANES
    count = 2 * SUB // step
    for n in range(count):
        cols = pl.ds(n * step, step)
        row_ref[:, cols] = jnp.dot(
            left_ref[...], twin_ref[:, cols], preferred_element_type=F32
        ).astype(BF)
    for n in range(count):
        cols = pl.ds(n * step, step)
        half = pl.ds(n * LANES, LANES)
        got = jnp.dot(row_ref[...], right_ref[:, cols], preferred_element_type=F32)
        real, imag = got[:, :LANES], got[:, LANES:]
        screen_real = first_ref[0, :, half].astype(F32)
        screen_imag = first_ref[1, :, half].astype(F32)
        new_real = (real * screen_real - imag * screen_imag).astype(BF)
        new_imag = (real * screen_imag + imag * screen_real).astype(BF)
        lower = pl.ds(n * step, LANES)
        upper = pl.ds(n * step + LANES, LANES)
        twin_ref[:SUB, lower] = new_real
        twin_ref[:SUB, upper] = new_imag
        twin_ref[SUB:, lower] = new_imag
        twin_ref[SUB:, upper] = -new_real
    for n in range(count):
        cols = pl.ds(n * step, step)
        row_ref[:, cols] = jnp.dot(
            left_ref[...], twin_ref[:, cols], preferred_element_type=F32
        ).astype(BF)
    tile_ref[TILES] = jnp.zeros((WIN, LANES), BF)
    for n in range(count):
        got = lax.dot_general(
            row_ref[...],
            right_ref[pl.ds(n * step, step), :],
            (((1,), (1,)), ((), ())),
            preferred_element_type=F32,
        )
        cols = pl.ds(n * LANES, LANES)
        screen_real = second_ref[0, :, cols].astype(F32)
        screen_imag = second_ref[1, :, cols].astype(F32)
        real_turned, imag_turned = swap_halves(screen_real), swap_halves(screen_imag)
        low = low_half(screen_real.shape)
        for h in range(2):
            part = got[:, h * LANES : (h + 1) * LANES]
            if h == 0:
                keep = jnp.where(low, screen_real, real_turned)
                cross = jnp.where(low, -screen_imag, imag_turned)
            else:
                keep = jnp.where(low, real_turned, screen_real)
                cross = jnp.where(low, -imag_turned, screen_imag)
            done = (part * keep + swap_halves(part) * cross).astype(BF)
            t = 2 * n + h
            tile_ref[t * SIDE : (t + 1) * SIDE] = done.reshape(SIDE, WIN, LANES)

    def cut(i, carry):
        tag = tags_ref[i]
        source = i // SLOTS
        slot = i % SLOTS
        for q in range(NX):
            out_ref[source * NX + q, slot] = tile_ref[tag, pl.ds(q * QUARTER, QUARTER), :]
        return carry

    lax.fori_loop(0, SOURCES * SLOTS, cut, 0, unroll=4)


def add_slots(rows_ref, slots_ref, accs):
    def step(d, carry):
        for cap in range(CAP):
            for j in range(NZ):
                slot = j * CAP + cap
                row = rows_ref[d * SLOTS + slot]
                accs[j][row] += slots_ref[d, slot].astype(F32)
        return carry

    lax.fori_loop(0, PEERS, step, 0)


def sum_first_kernel(rows_ref, slots_ref, *accs):
    for acc in accs:
        acc[...] = jnp.zeros(acc.shape, F32)
    add_slots(rows_ref, slots_ref, accs)


def sum_second_kernel(rows_ref, slots_ref, *refs):
    before, outs, accs = refs[:NZ], refs[NZ : 2 * NZ], refs[2 * NZ :]
    for acc, start in zip(accs, before):
        acc[...] = start[...]
    add_slots(rows_ref, slots_ref, accs)
    for acc, out in zip(accs, outs):
        out[...] = acc[:WIN].astype(BF)


def last_kernel(where_ref, table_ref, *refs):
    blocks, out_ref, tile_ref = refs[:NX], refs[NX], refs[NX + 1]
    count = WIN // NX
    for s in range(NX):
        q = (where_ref[0] + NX - s) % NX
        rows = pl.ds(pl.multiple_of(q * QUARTER, QUARTER), QUARTER)
        for w in range(count):
            tile_ref[w, rows, :] = blocks[s][w].astype(F32)
    for j in range(count // 2):
        ends = []
        for h in range(2):
            both = jnp.dot(
                table_ref[...],
                tile_ref[2 * j + h],
                precision=lax.Precision.HIGHEST,
                preferred_element_type=F32,
            )
            turned = swap_halves(both[WIN:])
            ends.append(both[:WIN] + jnp.where(low_half(turned.shape), -turned, turned))
        even, odd = ends
        low = low_half(even.shape)
        cols = pl.ds(j * LANES, LANES)
        out_ref[0, :, cols] = jnp.where(low, even, swap_halves(odd))
        out_ref[1, :, cols] = jnp.where(low, swap_halves(even), odd)


VMEM = pl.BlockSpec(memory_space=pltpu.VMEM)
SMEM = pl.BlockSpec(memory_space=pltpu.SMEM)


def call(kernel, specs, out, scratch=(), flops=0, moved=0):
    outs = jax.tree.map(lambda _: VMEM, out)
    return pl.pallas_call(
        kernel,
        in_specs=list(specs),
        out_specs=outs,
        out_shape=out,
        scratch_shapes=list(scratch),
        cost_estimate=pl.CostEstimate(flops=flops, bytes_accessed=moved, transcendentals=0),
        compiler_params=pltpu.CompilerParams(vmem_limit_bytes=48 << 20),
    )


def shift(value, axis, by):
    size = lax.axis_size(axis)
    return lax.ppermute(value, axis, [(i, (i + by) % size) for i in range(size)])


def pick(rows, index):
    hit = index[:, None] == jnp.arange(rows.shape[0], dtype=jnp.int32)[None, :]
    return jnp.sum(jnp.where(hit[:, :, None], rows[None], 0), axis=1)


def flip(value, axis, bit):
    size = lax.axis_size(axis)
    return lax.ppermute(value, axis, [(i, i ^ bit) for i in range(size)])


def exchange_codes(codes, z, x):
    table = codes
    for bit in (1, 2, 4):
        other = flip(table, "z", bit)
        table = jnp.concatenate([table, other], 0)
    table = lax.dynamic_index_in_dim(table.reshape(NZ, CAP, NZ, -1), z, 2, keepdims=False)
    table = pick(table.reshape(NZ, -1), (z + jnp.arange(NZ, dtype=jnp.int32)) % NZ ^ z).reshape(1, -1)
    every = [table]
    for step in range(1, NX):
        every.append(shift(table, "x", step))
    table = jnp.concatenate(every, 0)
    table = pick(table, (x - jnp.arange(NX, dtype=jnp.int32)) % NX)
    return table.reshape(NX, NZ, CAP, SOURCES, LOCAL)


def gather_up(own):
    half = WIN // 2
    down, up = [own], [own]
    for _ in range(3):
        up.append(shift(up[-1], "z", 1))
        down.append(shift(down[-1], "z", -1))
    low = shift(up[3][:half], "z", 1)
    high = shift(down[3][half:], "z", -1)
    return down + up[:0:-1] + [low, high]


def add(*terms):
    return sum(t.astype(F32) for t in terms).astype(BF)


def sum_up(parts):
    half = WIN // 2
    low = shift(parts[4][:half], "z", 1)
    high = shift(parts[4][half:], "z", -1)
    up = jnp.concatenate([add(parts[3][:half], low), parts[3][half:]], 0)
    down = jnp.concatenate([parts[5][:half], add(parts[5][half:], high)], 0)
    up, down = shift(up, "z", 1), shift(down, "z", -1)
    up, down = shift(add(parts[2], up), "z", 1), shift(add(parts[6], down), "z", -1)
    up, down = shift(add(parts[1], up), "z", 1), shift(add(parts[7], down), "z", -1)
    return add(parts[0], up, down)


def work(strip, screen_first, screen_second, owners, live, place):
    z, x = lax.axis_index("z"), lax.axis_index("x")
    plane = ("y", "k", "x")
    block = jax.ShapeDtypeStruct((WIN, QUARTER, LANES), BF)
    own = call(
        front_kernel, [SMEM, VMEM, VMEM], block, flops=2 * 32 * 128 * 4096, moved=2 << 20
    )(x.reshape(1), jnp.asarray(front_table()), strip)
    blocks = gather_up(own)

    codes = call(
        codes_kernel,
        [VMEM] * 3,
        jax.ShapeDtypeStruct((1, NZ * SOURCES * LOCAL * CAP), jnp.int32),
        flops=1 << 20,
        moved=1 << 12,
    )(owners, live, place)
    codes = exchange_codes(codes, z, x)
    codes = codes.transpose(4, 3, 0, 1, 2)
    dead = codes < 0
    rows = jnp.where(dead, WIN, codes // TILES).reshape(LOCAL, PEERS * SLOTS)
    taken = jnp.minimum(rows, WIN - 1)
    tags = codes % TILES
    tags = jnp.where(dead, TILES, tags % SIDE * SIDE + tags // SIDE)
    tags = tags.reshape(LOCAL, PEERS, SLOTS).transpose(1, 0, 2).reshape(PEERS, 1, LOCAL * SLOTS)
    extra = jnp.pad(tags.astype(BF), ((0, 0), (0, QUARTER - 1), (0, LANES - LOCAL * SLOTS)))

    left, right = jnp.asarray(left_table()), jnp.asarray(right_table())
    returned = []
    for part in range(LOCAL):
        first = part == 0
        sent = call(
            functools.partial(pack_kernel, first),
            [SMEM] + [VMEM] * (10 if first else 9),
            jax.ShapeDtypeStruct((PEERS, SLOTS + first, QUARTER, LANES), BF),
            scratch=[pltpu.VMEM((WIN, QUARTER, LANES), BF)],
            flops=1 << 28,
            moved=4 << 20,
        )(taken[part], *blocks, *([extra] if first else []))
        got = lax.all_to_all(sent, plane, split_axis=0, concat_axis=0, tiled=True)
        if first:
            spots = got.reshape(SOURCES, NX, SLOTS + 1, QUARTER, LANES)
            spots = spots[:, 0, SLOTS, 0, : LOCAL * SLOTS].astype(jnp.int32)
            spots = spots.reshape(SOURCES, LOCAL, SLOTS).transpose(1, 0, 2)
            spots = spots.reshape(LOCAL, SOURCES * SLOTS)
        done = call(
            subgrid_kernel,
            [SMEM] + [VMEM] * 5,
            jax.ShapeDtypeStruct((PEERS, SLOTS, QUARTER, LANES), BF),
            scratch=[
                pltpu.VMEM((TILES + 1, WIN, LANES), F32),
                pltpu.VMEM((2 * SUB, 2 * SUB), BF),
                pltpu.VMEM((SUB, 2 * SUB), BF),
                pltpu.VMEM((TILES + 1, WIN, LANES), BF),
            ],
            flops=8 * 2 * SUB * SUB * SUB * 2,
            moved=10 << 20,
        )(spots[part], left, right, screen_first, screen_second, got)
        done = lax.all_to_all(done, plane, split_axis=0, concat_axis=0, tiled=True)
        returned.append(done)
    acc = [jax.ShapeDtypeStruct((WIN + 1, QUARTER, LANES), F32)] * NZ
    partial = call(
        sum_first_kernel, [SMEM, VMEM], acc, flops=1 << 28, moved=6 << 20
    )(rows[0], returned[0])
    parts = call(
        sum_second_kernel,
        [SMEM, VMEM] + [VMEM] * NZ,
        [block] * NZ,
        scratch=[pltpu.VMEM((WIN + 1, QUARTER, LANES), F32)] * NZ,
        flops=1 << 28,
        moved=8 << 20,
    )(rows[1], returned[1], *partial)
    mine = sum_up(parts)
    count = WIN // NX
    pieces = []
    for s in range(NX):
        piece = lax.dynamic_slice_in_dim(mine, (x + s) % NX * count, count, 0)
        pieces.append(shift(piece, "x", s) if s else piece)
    return call(
        last_kernel,
        [SMEM] + [VMEM] * (1 + NX),
        jax.ShapeDtypeStruct((2, WIN, count * WIN), F32),
        scratch=[pltpu.VMEM((count, WIN, LANES), F32)],
        flops=1 << 28,
        moved=1 << 20,
    )(x.reshape(1), jnp.asarray(last_table()), *pieces)


def solution(mesh):
    fine = Mesh(mesh.devices.reshape(NZ, NY, NK, NX), ("z", "y", "k", "x"))
    facet = ("z", "y", "k")
    entry = P("x", facet, None)
    return jax.shard_map(
        work,
        mesh=fine,
        in_specs=(P(None, None, facet), P(), P(), entry, entry, entry),
        out_specs=P(None, None, facet + ("x",)),
        check_vma=False,
    )
```

```python
import functools
import math

import jax
import jax.numpy as jnp
import numpy as np
from jax import lax
from jax.experimental import pallas as pl
from jax.experimental.pallas import tpu as pltpu
from jax.sharding import Mesh, PartitionSpec as P

NZ, NY, NK, NX = 8, 4, 2, 4
WIN = 64
QUARTER = WIN // NX
SUB = 512
SIDE = SUB // WIN
TILES = SIDE * SIDE
CAP = 2
LOCAL = 2
SOURCES = NY * NK
PEERS = SOURCES * NX
SLOTS = NZ * CAP
LANES = 128
BF, F32 = jnp.bfloat16, jnp.float32


def dft(length):
    index = np.arange(length)
    angle = ((index[:, None] * index[None, :]) % length).astype(np.float32) * np.float32(
        2.0 * math.pi / length
    )
    scale = np.float32(1.0 / math.sqrt(length))
    return (
        (np.cos(angle) * scale).astype(np.float32),
        (-np.sin(angle) * scale).astype(np.float32),
    )


def front_table():
    real, imag = dft(WIN)
    both = np.stack(
        [np.concatenate([real, -imag], 1), np.concatenate([imag, real], 1)]
    )
    cut = both.reshape(2, NX, QUARTER, 2 * WIN).transpose(1, 0, 2, 3)
    return cut.reshape(NX, 2 * QUARTER, 2 * WIN).astype(BF)


def left_table():
    real, imag = dft(SUB)
    return np.concatenate([real, imag], 1).astype(BF)


def right_table():
    real, imag = dft(SUB)
    full = np.stack([np.stack([real, imag]), np.stack([-imag, real])])
    full = full.reshape(2, 2, SIDE, WIN, SUB // LANES, LANES)
    return full.transpose(2, 0, 3, 4, 1, 5).reshape(2 * SUB, 2 * SUB).astype(BF)


def last_table():
    real, imag = dft(WIN)
    rest = np.concatenate([real, -imag], 0).astype(np.float32)
    terms = []
    for _ in range(3):
        terms.append(rest.astype(BF))
        rest = rest - terms[-1].astype(np.float32)
    return np.concatenate(terms, 1)


def swap_halves(x):
    return pltpu.roll(x, WIN, x.ndim - 1)


def low_half(shape):
    return lax.broadcasted_iota(jnp.int32, shape, len(shape) - 1) < WIN


def front_kernel(where_ref, table_ref, strip_ref, owner_ref, live_ref, place_ref, out_ref, codes_ref):
    codes_kernel(owner_ref, live_ref, place_ref, codes_ref)
    table = table_ref[where_ref[0]]
    for j in range(WIN // 2):
        cols = pl.ds(j * LANES, LANES)
        block = jnp.concatenate([strip_ref[0, :, cols], strip_ref[1, :, cols]], 0)
        both = jnp.dot(table, block, preferred_element_type=F32)
        real, imag = both[:QUARTER], both[QUARTER:]
        low = low_half(real.shape)
        out_ref[2 * j] = jnp.where(low, real, swap_halves(imag)).astype(BF)
        out_ref[2 * j + 1] = jnp.where(low, swap_halves(real), imag).astype(BF)


def codes_kernel(owner_ref, live_ref, place_ref, out_ref):
    shape = (NZ * SOURCES * LOCAL, WIN)
    subgrid = lax.broadcasted_iota(jnp.int32, shape, 0)
    window = lax.broadcasted_iota(jnp.int32, shape, 1)
    count = jnp.zeros(shape, F32)
    which = jnp.zeros(shape, jnp.int32)
    tile = jnp.zeros(shape, jnp.int32)
    for k in range(3):
        hit = owner_ref[k] == subgrid
        used = hit & (live_ref[k] == 1)
        count += jnp.where(hit, 1.0, 0.0)
        which += jnp.where(used, window + 1, 0)
        tile += jnp.where(used, place_ref[k], 0)
    square = (WIN, WIN)
    earlier = lax.broadcasted_iota(jnp.int32, square, 0) < lax.broadcasted_iota(
        jnp.int32, square, 1
    )
    rank = jnp.dot(
        count.astype(BF), jnp.where(earlier, 1.0, 0.0).astype(BF), preferred_element_type=F32
    )
    ones = jnp.ones((8, WIN), BF)

    def as_row(value):
        return lax.dot_general(
            ones, value.astype(F32).astype(BF), (((1,), (1,)), ((), ())),
            preferred_element_type=F32,
        )[:1].astype(jnp.int32)

    for cap in range(CAP):
        mine = rank == float(cap)
        number = as_row(jnp.where(mine, which, 0))
        code = (number - 1) * TILES + as_row(jnp.where(mine, tile, 0))
        out_ref[:, cap * shape[0] : (cap + 1) * shape[0]] = jnp.where(number > 0, code, -1)


def pack_kernel(extra, rows_ref, *refs):
    blocks, out_ref = list(refs[:9]), refs[-2]
    middle_ref = refs[-1]
    middle_ref[: WIN // 2] = blocks[7][...]
    middle_ref[WIN // 2 :] = blocks[8][...]
    blocks = blocks[:4] + [middle_ref] + blocks[4:7]

    def step(d, carry):
        for j in range(NZ):
            for cap in range(CAP):
                slot = j * CAP + cap
                out_ref[d, slot] = blocks[j][rows_ref[d * SLOTS + slot]]
        if extra:
            out_ref[d, SLOTS] = refs[9][d]
        return carry

    lax.fori_loop(0, PEERS, step, 0, unroll=2)


def subgrid_kernel(
    tags_ref, left_ref, right_ref, first_ref, second_ref, slabs_ref, out_ref,
    acc_ref, twin_ref, row_ref, tile_ref,
):
    acc_ref[...] = jnp.zeros(acc_ref.shape, F32)

    def embed(i, carry):
        tag = tags_ref[i]
        source = i // SLOTS
        slot = i % SLOTS
        for q in range(NX):
            rows = pl.ds(q * QUARTER, QUARTER)
            acc_ref[tag, rows, :] += slabs_ref[source * NX + q, slot].astype(F32)
        return carry

    lax.fori_loop(0, SOURCES * SLOTS, embed, 0, unroll=4)

    for t in range(SIDE):
        cols = pl.ds(t * LANES, LANES)
        panel = acc_ref[t * SIDE : (t + 1) * SIDE].reshape(SUB, LANES)
        turned = swap_halves(panel)
        twin_ref[:SUB, cols] = panel.astype(BF)
        twin_ref[SUB:, cols] = jnp.where(low_half(panel.shape), -turned, turned).astype(BF)

    step = 2 * LANES
    count = 2 * SUB // step
    for n in range(count):
        cols = pl.ds(n * step, step)
        row_ref[:, cols] = jnp.dot(
            left_ref[...], twin_ref[:, cols], preferred_element_type=F32
        ).astype(BF)
    for n in range(count):
        cols = pl.ds(n * step, step)
        half = pl.ds(n * LANES, LANES)
        got = jnp.dot(row_ref[...], right_ref[:, cols], preferred_element_type=F32)
        real, imag = got[:, :LANES], got[:, LANES:]
        screen_real = first_ref[0, :, half].astype(F32)
        screen_imag = first_ref[1, :, half].astype(F32)
        new_real = (real * screen_real - imag * screen_imag).astype(BF)
        new_imag = (real * screen_imag + imag * screen_real).astype(BF)
        lower = pl.ds(n * step, LANES)
        upper = pl.ds(n * step + LANES, LANES)
        twin_ref[:SUB, lower] = new_real
        twin_ref[:SUB, upper] = new_imag
        twin_ref[SUB:, lower] = new_imag
        twin_ref[SUB:, upper] = -new_real
    for n in range(count):
        cols = pl.ds(n * step, step)
        row_ref[:, cols] = jnp.dot(
            left_ref[...], twin_ref[:, cols], preferred_element_type=F32
        ).astype(BF)
    tile_ref[TILES] = jnp.zeros((WIN, LANES), BF)
    for n in range(count):
        got = lax.dot_general(
            row_ref[...],
            right_ref[pl.ds(n * step, step), :],
            (((1,), (1,)), ((), ())),
            preferred_element_type=F32,
        )
        cols = pl.ds(n * LANES, LANES)
        screen_real = second_ref[0, :, cols].astype(F32)
        screen_imag = second_ref[1, :, cols].astype(F32)
        real_turned, imag_turned = swap_halves(screen_real), swap_halves(screen_imag)
        low = low_half(screen_real.shape)
        for h in range(2):
            part = got[:, h * LANES : (h + 1) * LANES]
            if h == 0:
                keep = jnp.where(low, screen_real, real_turned)
                cross = jnp.where(low, -screen_imag, imag_turned)
            else:
                keep = jnp.where(low, real_turned, screen_real)
                cross = jnp.where(low, -imag_turned, screen_imag)
            done = (part * keep + swap_halves(part) * cross).astype(BF)
            t = 2 * n + h
            tile_ref[t * SIDE : (t + 1) * SIDE] = done.reshape(SIDE, WIN, LANES)

    def cut(i, carry):
        tag = tags_ref[i]
        source = i // SLOTS
        slot = i % SLOTS
        for q in range(NX):
            out_ref[source * NX + q, slot] = tile_ref[tag, pl.ds(q * QUARTER, QUARTER), :]
        return carry

    lax.fori_loop(0, SOURCES * SLOTS, cut, 0, unroll=4)


def add_slots(rows_ref, slots_ref, accs):
    def step(d, carry):
        for cap in range(CAP):
            for j in range(NZ):
                slot = j * CAP + cap
                row = rows_ref[d * SLOTS + slot]
                accs[j][row] += slots_ref[d, slot].astype(F32)
        return carry

    lax.fori_loop(0, PEERS, step, 0)


def sum_first_kernel(rows_ref, slots_ref, *accs):
    for acc in accs:
        acc[...] = jnp.zeros(acc.shape, F32)
    add_slots(rows_ref, slots_ref, accs)


def sum_second_kernel(rows_ref, slots_ref, *refs):
    before, outs, accs = refs[:NZ], refs[NZ : 2 * NZ], refs[2 * NZ :]
    for acc, start in zip(accs, before):
        acc[...] = start[...]
    add_slots(rows_ref, slots_ref, accs)
    for acc, out in zip(accs, outs):
        out[...] = acc[:WIN].astype(BF)


def last_kernel(where_ref, table_ref, *refs):
    blocks, out_ref, tile_ref = refs[:NX], refs[NX], refs[NX + 1]
    count = WIN // NX
    for s in range(NX):
        q = (where_ref[0] + NX - s) % NX
        rows = pl.ds(pl.multiple_of(q * QUARTER, QUARTER), QUARTER)
        for w in range(count):
            tile_ref[w, rows, :] = blocks[s][w]
    for j in range(count // 2):
        ends = []
        for h in range(2):
            tile = tile_ref[2 * j + h]
            both = jnp.dot(
                table_ref[...],
                jnp.concatenate([tile] * 3, 0),
                preferred_element_type=F32,
            )
            turned = swap_halves(both[WIN:])
            ends.append(both[:WIN] + jnp.where(low_half(turned.shape), -turned, turned))
        even, odd = ends
        low = low_half(even.shape)
        cols = pl.ds(j * LANES, LANES)
        out_ref[0, :, cols] = jnp.where(low, even, swap_halves(odd))
        out_ref[1, :, cols] = jnp.where(low, swap_halves(even), odd)


VMEM = pl.BlockSpec(memory_space=pltpu.VMEM)
SMEM = pl.BlockSpec(memory_space=pltpu.SMEM)
FRONT_LIMIT = (64 << 20) - (256 << 10)


def call(kernel, specs, out, scratch=(), flops=0, moved=0, limit=48 << 20):
    outs = jax.tree.map(lambda _: VMEM, out)
    return pl.pallas_call(
        kernel,
        in_specs=list(specs),
        out_specs=outs,
        out_shape=out,
        scratch_shapes=list(scratch),
        cost_estimate=pl.CostEstimate(flops=flops, bytes_accessed=moved, transcendentals=0),
        compiler_params=pltpu.CompilerParams(vmem_limit_bytes=limit),
    )


def shift(value, axis, by):
    size = lax.axis_size(axis)
    return lax.ppermute(value, axis, [(i, (i + by) % size) for i in range(size)])


def pick(rows, index):
    hit = index[:, None] == jnp.arange(rows.shape[0], dtype=jnp.int32)[None, :]
    return jnp.sum(jnp.where(hit[:, :, None], rows[None], 0), axis=1)


def flip(value, axis, bit):
    size = lax.axis_size(axis)
    return lax.ppermute(value, axis, [(i, i ^ bit) for i in range(size)])


def exchange_codes(codes, z, x):
    table = codes
    for bit in (1, 2, 4):
        other = flip(table, "z", bit)
        table = jnp.concatenate([table, other], 0)
    table = lax.dynamic_index_in_dim(table.reshape(NZ, CAP, NZ, -1), z, 2, keepdims=False)
    table = pick(table.reshape(NZ, -1), (z + jnp.arange(NZ, dtype=jnp.int32)) % NZ ^ z).reshape(1, -1)
    every = [table]
    for step in range(1, NX):
        every.append(shift(table, "x", step))
    table = jnp.concatenate(every, 0)
    table = pick(table, (x - jnp.arange(NX, dtype=jnp.int32)) % NX)
    return table.reshape(NX, NZ, CAP, SOURCES, LOCAL)


def gather_up(own):
    half = WIN // 2
    down, up = [own], [own]
    for _ in range(3):
        up.append(shift(up[-1], "z", 1))
        down.append(shift(down[-1], "z", -1))
    low = shift(up[3][:half], "z", 1)
    high = shift(down[3][half:], "z", -1)
    return down + up[:0:-1] + [low, high]


def add(*terms):
    return sum(t.astype(F32) for t in terms).astype(BF)


def sum_up(parts):
    half = WIN // 2
    low = shift(parts[4][:half], "z", 1)
    high = shift(parts[4][half:], "z", -1)
    up = jnp.concatenate([add(parts[3][:half], low), parts[3][half:]], 0)
    down = jnp.concatenate([parts[5][:half], add(parts[5][half:], high)], 0)
    up, down = shift(up, "z", 1), shift(down, "z", -1)
    up, down = shift(add(parts[2], up), "z", 1), shift(add(parts[6], down), "z", -1)
    up, down = shift(add(parts[1], up), "z", 1), shift(add(parts[7], down), "z", -1)
    return add(parts[0], up, down)


def work(strip, screen_first, screen_second, owners, live, place):
    z, x = lax.axis_index("z"), lax.axis_index("x")
    plane = ("y", "k", "x")
    block = jax.ShapeDtypeStruct((WIN, QUARTER, LANES), BF)
    own, codes = call(
        front_kernel,
        [SMEM] + [VMEM] * 5,
        [block, jax.ShapeDtypeStruct((1, NZ * SOURCES * LOCAL * CAP), jnp.int32)],
        flops=2 * 32 * 128 * 4096,
        moved=2 << 20,
        limit=FRONT_LIMIT,
    )(
        x.reshape(1),
        jnp.asarray(front_table()),
        strip,
        *(a.transpose(2, 0, 1) for a in (owners, live, place)),
    )
    blocks = gather_up(own)
    codes = exchange_codes(codes, z, x)
    codes = codes.transpose(4, 3, 0, 1, 2)
    dead = codes < 0
    rows = jnp.where(dead, WIN, codes // TILES).reshape(LOCAL, PEERS * SLOTS)
    taken = jnp.minimum(rows, WIN - 1)
    tags = codes % TILES
    tags = jnp.where(dead, TILES, tags % SIDE * SIDE + tags // SIDE)
    tags = tags.reshape(LOCAL, PEERS, SLOTS).transpose(1, 0, 2).reshape(PEERS, 1, LOCAL * SLOTS)
    extra = jnp.pad(tags.astype(BF), ((0, 0), (0, QUARTER - 1), (0, LANES - LOCAL * SLOTS)))

    left, right = jnp.asarray(left_table()), jnp.asarray(right_table())
    returned = []
    for part in range(LOCAL):
        first = part == 0
        sent = call(
            functools.partial(pack_kernel, first),
            [SMEM] + [VMEM] * (10 if first else 9),
            jax.ShapeDtypeStruct((PEERS, SLOTS + first, QUARTER, LANES), BF),
            scratch=[pltpu.VMEM((WIN, QUARTER, LANES), BF)],
            flops=1 << 28,
            moved=4 << 20,
        )(taken[part], *blocks, *([extra] if first else []))
        got = lax.all_to_all(sent, plane, split_axis=0, concat_axis=0, tiled=True)
        if first:
            spots = got.reshape(SOURCES, NX, SLOTS + 1, QUARTER, LANES)
            spots = spots[:, 0, SLOTS, 0, : LOCAL * SLOTS].astype(jnp.int32)
            spots = spots.reshape(SOURCES, LOCAL, SLOTS).transpose(1, 0, 2)
            spots = spots.reshape(LOCAL, SOURCES * SLOTS)
        done = call(
            subgrid_kernel,
            [SMEM] + [VMEM] * 5,
            jax.ShapeDtypeStruct((PEERS, SLOTS, QUARTER, LANES), BF),
            scratch=[
                pltpu.VMEM((TILES + 1, WIN, LANES), F32),
                pltpu.VMEM((2 * SUB, 2 * SUB), BF),
                pltpu.VMEM((SUB, 2 * SUB), BF),
                pltpu.VMEM((TILES + 1, WIN, LANES), BF),
            ],
            flops=8 * 2 * SUB * SUB * SUB * 2,
            moved=10 << 20,
        )(spots[part], left, right, screen_first, screen_second, got)
        done = lax.all_to_all(done, plane, split_axis=0, concat_axis=0, tiled=True)
        returned.append(done)
    acc = [jax.ShapeDtypeStruct((WIN + 1, QUARTER, LANES), F32)] * NZ
    partial = call(
        sum_first_kernel, [SMEM, VMEM], acc, flops=1 << 28, moved=6 << 20
    )(rows[0], returned[0])
    parts = call(
        sum_second_kernel,
        [SMEM, VMEM] + [VMEM] * NZ,
        [block] * NZ,
        scratch=[pltpu.VMEM((WIN + 1, QUARTER, LANES), F32)] * NZ,
        flops=1 << 28,
        moved=8 << 20,
    )(rows[1], returned[1], *partial)
    mine = sum_up(parts)
    count = WIN // NX
    pieces = []
    for s in range(NX):
        piece = lax.dynamic_slice_in_dim(mine, (x + s) % NX * count, count, 0)
        pieces.append(shift(piece, "x", s) if s else piece)
    return call(
        last_kernel,
        [SMEM] + [VMEM] * (1 + NX),
        jax.ShapeDtypeStruct((2, WIN, count * WIN), F32),
        scratch=[pltpu.VMEM((count, WIN, LANES), BF)],
        flops=1 << 28,
        moved=1 << 20,
    )(x.reshape(1), jnp.asarray(last_table()), *pieces)


def solution(mesh):
    fine = Mesh(mesh.devices.reshape(NZ, NY, NK, NX), ("z", "y", "k", "x"))
    facet = ("z", "y", "k")
    entry = P("x", facet, None)
    return jax.shard_map(
        work,
        mesh=fine,
        in_specs=(P(None, None, facet), P(), P(), entry, entry, entry),
        out_specs=P(None, None, facet + ("x",)),
        check_vma=False,
    )
```

```python
import functools
import math

import jax
import jax.numpy as jnp
import numpy as np
from jax import lax
from jax.experimental import pallas as pl
from jax.experimental.pallas import tpu as pltpu
from jax.sharding import Mesh, PartitionSpec as P

NZ, NY, NK, NX = 8, 4, 2, 4
WIN = 64
QUARTER = WIN // NX
SUB = 512
SIDE = SUB // WIN
TILES = SIDE * SIDE
CAP = 2
LOCAL = 2
SOURCES = NY * NK
PEERS = SOURCES * NX
SLOTS = NZ * CAP
LANES = 128
BF, F32 = jnp.bfloat16, jnp.float32


def dft(length):
    index = np.arange(length)
    angle = ((index[:, None] * index[None, :]) % length).astype(np.float32) * np.float32(
        2.0 * math.pi / length
    )
    scale = np.float32(1.0 / math.sqrt(length))
    return (
        (np.cos(angle) * scale).astype(np.float32),
        (-np.sin(angle) * scale).astype(np.float32),
    )


def front_table():
    real, imag = dft(WIN)
    both = np.stack(
        [np.concatenate([real, -imag], 1), np.concatenate([imag, real], 1)]
    )
    cut = both.reshape(2, NX, QUARTER, 2 * WIN).transpose(1, 0, 2, 3)
    return cut.reshape(NX, 2 * QUARTER, 2 * WIN).astype(BF)


def left_table():
    real, imag = dft(SUB)
    return np.concatenate([real, imag], 1).astype(BF)


def right_table():
    real, imag = dft(SUB)
    full = np.stack([np.stack([real, imag]), np.stack([-imag, real])])
    full = full.reshape(2, 2, SIDE, WIN, SUB // LANES, LANES)
    return full.transpose(2, 0, 3, 4, 1, 5).reshape(2 * SUB, 2 * SUB).astype(BF)


def last_table():
    real, imag = dft(WIN)
    rest = np.concatenate([real, -imag], 0).astype(np.float32)
    terms = []
    for _ in range(3):
        terms.append(rest.astype(BF))
        rest = rest - terms[-1].astype(np.float32)
    return np.concatenate(terms, 1)


def swap_halves(x):
    return pltpu.roll(x, WIN, x.ndim - 1)


def low_half(shape):
    return lax.broadcasted_iota(jnp.int32, shape, len(shape) - 1) < WIN


def front_kernel(where_ref, table_ref, strip_ref, out_ref):
    table = table_ref[where_ref[0]]
    for j in range(WIN // 2):
        cols = pl.ds(j * LANES, LANES)
        block = jnp.concatenate([strip_ref[0, :, cols], strip_ref[1, :, cols]], 0)
        both = jnp.dot(table, block, preferred_element_type=F32)
        real, imag = both[:QUARTER], both[QUARTER:]
        low = low_half(real.shape)
        out_ref[2 * j] = jnp.where(low, real, swap_halves(imag)).astype(BF)
        out_ref[2 * j + 1] = jnp.where(low, swap_halves(real), imag).astype(BF)


def codes_kernel(owner_ref, live_ref, place_ref, out_ref):
    shape = (WIN, NZ * SOURCES * LOCAL)
    window = lax.broadcasted_iota(jnp.int32, shape, 0)
    subgrid = lax.broadcasted_iota(jnp.int32, shape, 1)
    count = jnp.zeros(shape, F32)
    value = jnp.zeros(shape, F32)
    for k in range(3):
        entry = (0, slice(None), slice(k, k + 1))
        hit = owner_ref[entry] == subgrid
        code = (window * TILES + place_ref[entry] + 1).astype(F32)
        count += jnp.where(hit, 1.0, 0.0)
        value += jnp.where(hit & (live_ref[entry] == 1), code, 0.0)
    square = (WIN, WIN)
    earlier = lax.broadcasted_iota(jnp.int32, square, 1) < lax.broadcasted_iota(
        jnp.int32, square, 0
    )
    rank = jnp.dot(
        jnp.where(earlier, 1.0, 0.0).astype(BF), count.astype(BF), preferred_element_type=F32
    )
    for cap in range(CAP):
        mine = jnp.sum(jnp.where(rank == float(cap), value, 0.0), axis=0, keepdims=True)
        out_ref[:, cap * shape[1] : (cap + 1) * shape[1]] = mine.astype(jnp.int32) - 1


def pack_kernel(extra, rows_ref, *refs):
    blocks, out_ref = list(refs[:9]), refs[-2]
    middle_ref = refs[-1]
    middle_ref[: WIN // 2] = blocks[7][...]
    middle_ref[WIN // 2 :] = blocks[8][...]
    blocks = blocks[:4] + [middle_ref] + blocks[4:7]

    def step(d, carry):
        for j in range(NZ):
            for cap in range(CAP):
                slot = j * CAP + cap
                out_ref[d, slot] = blocks[j][rows_ref[d * SLOTS + slot]]
        if extra:
            out_ref[d, SLOTS] = refs[9][d]
        return carry

    lax.fori_loop(0, PEERS, step, 0, unroll=2)


def subgrid_kernel(
    tags_ref, left_ref, right_ref, first_ref, second_ref, slabs_ref, out_ref,
    acc_ref, twin_ref, row_ref, tile_ref,
):
    acc_ref[...] = jnp.zeros(acc_ref.shape, F32)

    def embed(i, carry):
        tag = tags_ref[i]
        source = i // SLOTS
        slot = i % SLOTS
        for q in range(NX):
            rows = pl.ds(q * QUARTER, QUARTER)
            acc_ref[tag, rows, :] += slabs_ref[source * NX + q, slot].astype(F32)
        return carry

    lax.fori_loop(0, SOURCES * SLOTS, embed, 0, unroll=4)

    for t in range(SIDE):
        cols = pl.ds(t * LANES, LANES)
        panel = acc_ref[t * SIDE : (t + 1) * SIDE].reshape(SUB, LANES)
        turned = swap_halves(panel)
        twin_ref[:SUB, cols] = panel.astype(BF)
        twin_ref[SUB:, cols] = jnp.where(low_half(panel.shape), -turned, turned).astype(BF)

    step = 2 * LANES
    count = 2 * SUB // step
    for n in range(count):
        cols = pl.ds(n * step, step)
        row_ref[:, cols] = jnp.dot(
            left_ref[...], twin_ref[:, cols], preferred_element_type=F32
        ).astype(BF)
    for n in range(count):
        cols = pl.ds(n * step, step)
        half = pl.ds(n * LANES, LANES)
        got = jnp.dot(row_ref[...], right_ref[:, cols], preferred_element_type=F32)
        real, imag = got[:, :LANES], got[:, LANES:]
        screen_real = first_ref[0, :, half].astype(F32)
        screen_imag = first_ref[1, :, half].astype(F32)
        new_real = (real * screen_real - imag * screen_imag).astype(BF)
        new_imag = (real * screen_imag + imag * screen_real).astype(BF)
        lower = pl.ds(n * step, LANES)
        upper = pl.ds(n * step + LANES, LANES)
        twin_ref[:SUB, lower] = new_real
        twin_ref[:SUB, upper] = new_imag
        twin_ref[SUB:, lower] = new_imag
        twin_ref[SUB:, upper] = -new_real
    for n in range(count):
        cols = pl.ds(n * step, step)
        row_ref[:, cols] = jnp.dot(
            left_ref[...], twin_ref[:, cols], preferred_element_type=F32
        ).astype(BF)
    tile_ref[TILES] = jnp.zeros((WIN, LANES), BF)
    for n in range(count):
        got = lax.dot_general(
            row_ref[...],
            right_ref[pl.ds(n * step, step), :],
            (((1,), (1,)), ((), ())),
            preferred_element_type=F32,
        )
        cols = pl.ds(n * LANES, LANES)
        screen_real = second_ref[0, :, cols].astype(F32)
        screen_imag = second_ref[1, :, cols].astype(F32)
        real_turned, imag_turned = swap_halves(screen_real), swap_halves(screen_imag)
        low = low_half(screen_real.shape)
        for h in range(2):
            part = got[:, h * LANES : (h + 1) * LANES]
            if h == 0:
                keep = jnp.where(low, screen_real, real_turned)
                cross = jnp.where(low, -screen_imag, imag_turned)
            else:
                keep = jnp.where(low, real_turned, screen_real)
                cross = jnp.where(low, -imag_turned, screen_imag)
            done = (part * keep + swap_halves(part) * cross).astype(BF)
            t = 2 * n + h
            tile_ref[t * SIDE : (t + 1) * SIDE] = done.reshape(SIDE, WIN, LANES)

    def cut(i, carry):
        tag = tags_ref[i]
        source = i // SLOTS
        slot = i % SLOTS
        for q in range(NX):
            out_ref[source * NX + q, slot] = tile_ref[tag, pl.ds(q * QUARTER, QUARTER), :]
        return carry

    lax.fori_loop(0, SOURCES * SLOTS, cut, 0, unroll=4)


def add_slots(rows_ref, slots_ref, accs):
    def step(d, carry):
        for cap in range(CAP):
            for j in range(NZ):
                slot = j * CAP + cap
                row = rows_ref[d * SLOTS + slot]
                accs[j][row] += slots_ref[d, slot].astype(F32)
        return carry

    lax.fori_loop(0, PEERS, step, 0)


def sum_first_kernel(rows_ref, slots_ref, *accs):
    for acc in accs:
        acc[...] = jnp.zeros(acc.shape, F32)
    add_slots(rows_ref, slots_ref, accs)


def sum_second_kernel(rows_ref, slots_ref, *refs):
    before, outs, accs = refs[:NZ], refs[NZ : 2 * NZ], refs[2 * NZ :]
    for acc, start in zip(accs, before):
        acc[...] = start[...]
    add_slots(rows_ref, slots_ref, accs)
    for acc, out in zip(accs, outs):
        out[...] = acc[:WIN].astype(BF)


def last_kernel(where_ref, table_ref, *refs):
    blocks, out_ref, tile_ref = refs[: 3 * NX], refs[-2], refs[-1]
    count = WIN // NX
    for s in range(NX):
        q = (where_ref[0] + NX - s) % NX
        rows = pl.ds(pl.multiple_of(q * QUARTER, QUARTER), QUARTER)
        for w in range(count):
            terms = [block[w].astype(F32) for block in blocks[3 * s : 3 * s + 3]]
            tile_ref[w, rows, :] = (terms[0] + terms[1] + terms[2]).astype(BF)
    for j in range(count // 2):
        ends = []
        for h in range(2):
            tile = tile_ref[2 * j + h]
            both = jnp.dot(
                table_ref[...],
                jnp.concatenate([tile] * 3, 0),
                preferred_element_type=F32,
            )
            turned = swap_halves(both[WIN:])
            ends.append(both[:WIN] + jnp.where(low_half(turned.shape), -turned, turned))
        even, odd = ends
        low = low_half(even.shape)
        cols = pl.ds(j * LANES, LANES)
        out_ref[0, :, cols] = jnp.where(low, even, swap_halves(odd))
        out_ref[1, :, cols] = jnp.where(low, swap_halves(even), odd)


VMEM = pl.BlockSpec(memory_space=pltpu.VMEM)
SMEM = pl.BlockSpec(memory_space=pltpu.SMEM)


def call(kernel, specs, out, scratch=(), flops=0, moved=0):
    outs = jax.tree.map(lambda _: VMEM, out)
    return pl.pallas_call(
        kernel,
        in_specs=list(specs),
        out_specs=outs,
        out_shape=out,
        scratch_shapes=list(scratch),
        cost_estimate=pl.CostEstimate(flops=flops, bytes_accessed=moved, transcendentals=0),
        compiler_params=pltpu.CompilerParams(vmem_limit_bytes=48 << 20),
    )


def shift(value, axis, by):
    size = lax.axis_size(axis)
    return lax.ppermute(value, axis, [(i, (i + by) % size) for i in range(size)])


def pick(rows, index):
    hit = index[:, None] == jnp.arange(rows.shape[0], dtype=jnp.int32)[None, :]
    return jnp.sum(jnp.where(hit[:, :, None], rows[None], 0), axis=1)


def flip(value, axis, bit):
    size = lax.axis_size(axis)
    return lax.ppermute(value, axis, [(i, i ^ bit) for i in range(size)])


def exchange_codes(codes, z, x):
    table = codes
    for bit in (1, 2, 4):
        other = flip(table, "z", bit)
        table = jnp.concatenate([table, other], 0)
    table = lax.dynamic_index_in_dim(table.reshape(NZ, CAP, NZ, -1), z, 2, keepdims=False)
    table = pick(table.reshape(NZ, -1), (z + jnp.arange(NZ, dtype=jnp.int32)) % NZ ^ z).reshape(1, -1)
    every = [table]
    for step in range(1, NX):
        every.append(shift(table, "x", step))
    table = jnp.concatenate(every, 0)
    table = pick(table, (x - jnp.arange(NX, dtype=jnp.int32)) % NX)
    return table.reshape(NX, NZ, CAP, SOURCES, LOCAL)


def gather_up(own):
    half = WIN // 2
    down, up = [own], [own]
    for _ in range(3):
        up.append(shift(up[-1], "z", 1))
        down.append(shift(down[-1], "z", -1))
    low = shift(up[3][:half], "z", 1)
    high = shift(down[3][half:], "z", -1)
    return down + up[:0:-1] + [low, high]


def add(*terms):
    return sum(t.astype(F32) for t in terms).astype(BF)


def sum_up(parts):
    half = WIN // 2
    low = shift(parts[4][:half], "z", 1)
    high = shift(parts[4][half:], "z", -1)
    up = jnp.concatenate([add(parts[3][:half], low), parts[3][half:]], 0)
    down = jnp.concatenate([parts[5][:half], add(parts[5][half:], high)], 0)
    up, down = shift(up, "z", 1), shift(down, "z", -1)
    up, down = add(parts[2], up), add(parts[6], down)
    up, down = shift(up, "z", 1), shift(down, "z", -1)
    return parts[0], add(parts[1], up), add(parts[7], down)


def send(value, by_z, by_x):
    nz, nx = lax.axis_size("z"), lax.axis_size("x")
    pairs = [
        (z * nx + x, (z + by_z) % nz * nx + (x + by_x) % nx)
        for z in range(nz)
        for x in range(nx)
    ]
    return lax.ppermute(value, ("z", "x"), pairs)


def work(strip, screen_first, screen_second, owners, live, place):
    z, x = lax.axis_index("z"), lax.axis_index("x")
    plane = ("y", "k", "x")
    block = jax.ShapeDtypeStruct((WIN, QUARTER, LANES), BF)
    own = call(
        front_kernel, [SMEM, VMEM, VMEM], block, flops=2 * 32 * 128 * 4096, moved=2 << 20
    )(x.reshape(1), jnp.asarray(front_table()), strip)
    blocks = gather_up(own)

    codes = call(
        codes_kernel,
        [VMEM] * 3,
        jax.ShapeDtypeStruct((1, NZ * SOURCES * LOCAL * CAP), jnp.int32),
        flops=1 << 20,
        moved=1 << 12,
    )(owners, live, place)
    codes = exchange_codes(codes, z, x)
    codes = codes.transpose(4, 3, 0, 1, 2)
    dead = codes < 0
    rows = jnp.where(dead, WIN, codes // TILES).reshape(LOCAL, PEERS * SLOTS)
    taken = jnp.minimum(rows, WIN - 1)
    tags = codes % TILES
    tags = jnp.where(dead, TILES, tags % SIDE * SIDE + tags // SIDE)
    tags = tags.reshape(LOCAL, PEERS, SLOTS).transpose(1, 0, 2).reshape(PEERS, 1, LOCAL * SLOTS)
    extra = jnp.pad(tags.astype(BF), ((0, 0), (0, QUARTER - 1), (0, LANES - LOCAL * SLOTS)))

    left, right = jnp.asarray(left_table()), jnp.asarray(right_table())
    returned = []
    for part in range(LOCAL):
        first = part == 0
        sent = call(
            functools.partial(pack_kernel, first),
            [SMEM] + [VMEM] * (10 if first else 9),
            jax.ShapeDtypeStruct((PEERS, SLOTS + first, QUARTER, LANES), BF),
            scratch=[pltpu.VMEM((WIN, QUARTER, LANES), BF)],
            flops=1 << 28,
            moved=4 << 20,
        )(taken[part], *blocks, *([extra] if first else []))
        got = lax.all_to_all(sent, plane, split_axis=0, concat_axis=0, tiled=True)
        if first:
            spots = got.reshape(SOURCES, NX, SLOTS + 1, QUARTER, LANES)
            spots = spots[:, 0, SLOTS, 0, : LOCAL * SLOTS].astype(jnp.int32)
            spots = spots.reshape(SOURCES, LOCAL, SLOTS).transpose(1, 0, 2)
            spots = spots.reshape(LOCAL, SOURCES * SLOTS)
        done = call(
            subgrid_kernel,
            [SMEM] + [VMEM] * 5,
            jax.ShapeDtypeStruct((PEERS, SLOTS, QUARTER, LANES), BF),
            scratch=[
                pltpu.VMEM((TILES + 1, WIN, LANES), F32),
                pltpu.VMEM((2 * SUB, 2 * SUB), BF),
                pltpu.VMEM((SUB, 2 * SUB), BF),
                pltpu.VMEM((TILES + 1, WIN, LANES), BF),
            ],
            flops=8 * 2 * SUB * SUB * SUB * 2,
            moved=10 << 20,
        )(spots[part], left, right, screen_first, screen_second, got)
        done = lax.all_to_all(done, plane, split_axis=0, concat_axis=0, tiled=True)
        returned.append(done)
    acc = [jax.ShapeDtypeStruct((WIN + 1, QUARTER, LANES), F32)] * NZ
    partial = call(
        sum_first_kernel, [SMEM, VMEM], acc, flops=1 << 28, moved=6 << 20
    )(rows[0], returned[0])
    parts = call(
        sum_second_kernel,
        [SMEM, VMEM] + [VMEM] * NZ,
        [block] * NZ,
        scratch=[pltpu.VMEM((WIN + 1, QUARTER, LANES), F32)] * NZ,
        flops=1 << 28,
        moved=8 << 20,
    )(rows[1], returned[1], *partial)
    own, up, down = sum_up(parts)
    count = WIN // NX
    pieces = []
    for s in range(NX):
        first = (x + s) % NX * count
        kept = lax.dynamic_slice_in_dim(own, first, count, 0)
        if s:
            kept = shift(kept, "x", s)
        pieces.append(kept)
        pieces.append(send(lax.dynamic_slice_in_dim(up, first, count, 0), 1, s))
        pieces.append(send(lax.dynamic_slice_in_dim(down, first, count, 0), -1, s))
    return call(
        last_kernel,
        [SMEM] + [VMEM] * (1 + 3 * NX),
        jax.ShapeDtypeStruct((2, WIN, count * WIN), F32),
        scratch=[pltpu.VMEM((count, WIN, LANES), BF)],
        flops=1 << 28,
        moved=1 << 20,
    )(x.reshape(1), jnp.asarray(last_table()), *pieces)


def solution(mesh):
    fine = Mesh(mesh.devices.reshape(NZ, NY, NK, NX), ("z", "y", "k", "x"))
    facet = ("z", "y", "k")
    entry = P("x", facet, None)
    return jax.shard_map(
        work,
        mesh=fine,
        in_specs=(P(None, None, facet), P(), P(), entry, entry, entry),
        out_specs=P(None, None, facet + ("x",)),
        check_vma=False,
    )
```
